32 devices in a mesh: rep: 4 (over x, y), dp: 8 (over z, core).
Axes of the slice: x: 2, y: 2, z: 4, core: 2. Of those that a mesh axis runs over, the one named last changes fastest.
Arguments:
- x: bfloat16 [32, 2048, 896], P(('rep', 'dp')), parts along dimension 0
- dy: bfloat16 [32, 2048, 896], P(('rep', 'dp')), parts along dimension 0
- w_gate: bfloat16 [2, 896, 2304], replicated
- w_up: bfloat16 [2, 896, 2304], replicated
- w_down: bfloat16 [2, 2304, 896], replicated
- m_w_gate: float32 [2, 896, 2304], replicated
- m_w_up: float32 [2, 896, 2304], replicated
- m_w_down: float32 [2, 2304, 896], replicated
- v_w_gate: float32 [2, 896, 2304], replicated
- v_w_up: float32 [2, 896, 2304], replicated
- v_w_down: float32 [2, 2304, 896], replicated
Outputs:
- output 1: bfloat16 [8, 896, 2304], P('rep'), parts along dimension 0
- output 2: bfloat16 [8, 896, 2304], P('rep'), parts along dimension 0
- output 3: bfloat16 [8, 2304, 896], P('rep'), parts along dimension 0
- output 4: float32 [8, 896, 2304], P('rep'), parts along dimension 0
- output 5: float32 [8, 896, 2304], P('rep'), parts along dimension 0
- output 6: float32 [8, 2304, 896], P('rep'), parts along dimension 0
- output 7: float32 [8, 896, 2304], P('rep'), parts along dimension 0
- output 8: float32 [8, 896, 2304], P('rep'), parts along dimension 0
- output 9: float32 [8, 2304, 896], P('rep'), parts along dimension 0
There are 4 independent parts. The reference program is written for one: setup_inputs(seed, part) draws one part's arguments, and reference() takes and returns one part's arrays. A program takes and returns all parts, laid end to end along the dimension named above; an argument that names none is the same for every part.
All inputs are finite; a program needn't handle non-finite values.
Results may differ from the reference program's by a relative error of at most 0.02.
Values are sent between devices in bfloat16 or wider.
A program may use at most 2.5 GiB of HBM per device.

```python
import jax
import jax.numpy as jnp
from jax import lax

SEQUENCES = 8
TOKENS = 2048
D = 896
FF = 2304
LAYERS = 2
NAMES = ("w_gate", "w_up", "w_down")
SHAPES = {"w_gate": (LAYERS, D, FF), "w_up": (LAYERS, D, FF), "w_down": (LAYERS, FF, D)}


def bump(key, n, height):
    away = (jnp.arange(n, dtype=jnp.int32) - jax.random.randint(key, (), 0, n, jnp.int32)) % n
    return jnp.where(away < n // 8, height, 1.0)


def together(key, own, strength):
    shared = jax.random.normal(key, own.shape[1:], jnp.float32)
    return (own + strength * shared) * lax.rsqrt(1 + strength * strength)


def setup_inputs(seed: int = 0, part: int = 0) -> dict:
    kx, kdy, ka, kb, kz, kf, kh, kl, *keys = jax.random.split(jax.random.key(seed), 8 + 3 * len(NAMES))
    kx, kdy, ka, kb = (jax.random.fold_in(k, part) for k in (kx, kdy, ka, kb))
    kw, km, kv = (keys[i::3] for i in range(3))
    shape = (SEQUENCES, TOKENS, D)
    much_x, much_dy = jax.random.uniform(kz, (2,), jnp.float32, 0.0, 1.0)
    loud = 2.0 ** jax.random.uniform(jax.random.fold_in(kz, 1), (), jnp.float32, -1.0, 2.0)
    layers = 2.0 ** jax.random.uniform(kl, (LAYERS, 1, 1), jnp.float32, -1.0, 1.0)
    x = together(ka, jax.random.normal(kx, shape, jnp.float32), much_x) * bump(kf, D, 4.0)
    dy = together(kb, jax.random.normal(kdy, shape, jnp.float32), much_dy)
    drawn = {"x": x.astype(jnp.bfloat16), "dy": (loud * dy * (SEQUENCES * TOKENS) ** -0.5).astype(jnp.bfloat16)}
    for key, name in zip(kw, NAMES, strict=True):
        w = jax.random.normal(key, SHAPES[name], jnp.float32) * SHAPES[name][1] ** -0.5
        drawn[name] = (w * {"w_gate": 1.0, "w_up": bump(kh, FF, 4.0), "w_down": layers}[name]).astype(jnp.bfloat16)
    for key, name in zip(km, NAMES, strict=True):
        drawn[f"m_{name}"] = 0.1 * jax.random.normal(key, SHAPES[name], jnp.float32)
    for key, name in zip(kv, NAMES, strict=True):
        drawn[f"v_{name}"] = jax.random.uniform(key, SHAPES[name], jnp.float32, 0.005, 0.015)
    return drawn


def matmul(a, w):
    return jnp.dot(a, w, preferred_element_type=jnp.float32).astype(jnp.bfloat16)


def normed(h):
    wide = h.astype(jnp.float32)
    scale = lax.rsqrt(jnp.mean(wide**2, -1, keepdims=True) + 1e-6)
    return (wide * scale).astype(jnp.bfloat16)


def layer(h, w):
    a = normed(h)
    gate = jnp.dot(a, w["w_gate"], preferred_element_type=jnp.float32)
    up = jnp.dot(a, w["w_up"], preferred_element_type=jnp.float32)
    return h + matmul((jax.nn.silu(gate) * up).astype(jnp.bfloat16), w["w_down"])


def adamw(w, m, v, g):
    m = 0.9 * m + 0.1 * g
    v = 0.95 * v + 0.05 * g * g
    step = m * lax.rsqrt(v + 1e-8) + 0.1 * w
    return (w - 0.02 * step).astype(jnp.bfloat16), m, v


def stack(weights, h):
    return lax.scan(lambda h, w: (layer(h, w), None), h, weights)[0]


def reference(x, dy, w_gate, w_up, w_down, m_w_gate, m_w_up, m_w_down, v_w_gate, v_w_up, v_w_down):
    weights = dict(zip(NAMES, (w_gate, w_up, w_down), strict=True))

    def take(so_far, sequence):
        h, by_y = sequence
        _, back = jax.vjp(lambda w: stack(w, h), weights)
        return jax.tree.map(lambda total, term: total + term.astype(jnp.float32), so_far, back(by_y)[0]), None

    none_yet = {name: jnp.zeros(w.shape, jnp.float32) for name, w in weights.items()}
    by_weights, _ = lax.scan(take, none_yet, (x, dy))
    gradients = [by_weights[name].astype(jnp.bfloat16).astype(jnp.float32) for name in NAMES]
    new = [
        adamw(w.astype(jnp.float32), m, v, g)
        for w, m, v, g in zip((w_gate, w_up, w_down), (m_w_gate, m_w_up, m_w_down), (v_w_gate, v_w_up, v_w_down), gradients, strict=True)
    ]
    return tuple(one[which] for which in range(3) for one in new)
```

```python
import functools
import jax, jax.numpy as jnp
from jax import lax
from jax.experimental import pallas as pl
from jax.experimental.pallas import tpu as pltpu
BF, F32 = jnp.bfloat16, jnp.float32
T, D, FF = 2048, 896, 2304
C = 256
NCH = FF // C
HALF = 3 * D // 2
VL = 60 * 2**20
NT = (((1,), (1,)), ((), ()))

def dot(a, b, dims=(((1,), (0,)), ((), ()))):
    return lax.dot_general(a, b, dims, preferred_element_type=F32)

def cparams(**kw):
    return pltpu.CompilerParams(vmem_limit_bytes=VL, **kw)

VM = pl.BlockSpec(memory_space=pltpu.VMEM)
ANY = pl.BlockSpec(memory_space=pl.ANY)

def norm_scale(wide):
    return lax.rsqrt(jnp.mean(wide * wide, -1, keepdims=True) + 1e-6)

def fwd_body(x_hbm, dy_hbm, wg_ref, wu_ref, wd_hbm, h_hbm, a1_hbm, a1t_hbm, a0_hbm, a0t_hbm, dyt_hbm,
             x, dy, a0, a0t, dyt, hid, wd, h, a1, a1t, sem):
    j = pl.program_id(0)
    RT = 512
    def cin(src, dst, i): return pltpu.make_async_copy(src, dst, sem.at[i])
    def rows(i): return pl.ds(i * RT, RT)
    outs = lambda: [cin(a0, a0_hbm, 4), cin(a0t, a0t_hbm, 5), cin(dyt, dyt_hbm, 6)]
    @pl.when(j == 0)
    def _():
        for i in range(4):
            cin(x_hbm.at[rows(i)], x.at[rows(i)], 12 + i).start()
        cin(dy_hbm, dy, 1).start()
        cin(wd_hbm.at[0], wd, 2).start()
        for i in range(4):
            cin(x_hbm.at[rows(i)], x.at[rows(i)], 12 + i).wait()
            wide = x[rows(i), :].astype(F32)
            a = (wide * norm_scale(wide)).astype(BF)
            a0[rows(i), :] = a
            a0t[:, rows(i)] = a.T
        cin(dy_hbm, dy, 1).wait()
        for i in range(4):
            dyt[:, rows(i)] = dy[rows(i), :].T
        for c in outs(): c.start()
    cols = pl.ds(pl.multiple_of(j * C, C), C)
    for i in range(4):
        a = a0[rows(i), :]
        g = dot(a, wg_ref[0]); u = dot(a, wu_ref[0])
        hid[rows(i), cols] = (g * jax.nn.sigmoid(g) * u).astype(BF)
    @pl.when(j == NCH - 1)
    def _():
        cin(wd_hbm.at[0], wd, 2).wait()
        cs = []
        for i in range(8):
            r = pl.ds(i * 256, 256)
            o = dot(hid[r, :], wd[...]).astype(BF)
            y = x[r, :] + o
            h[r, :] = y
            wide = y.astype(F32)
            a = (wide * norm_scale(wide)).astype(BF)
            a1[r, :] = a
            a1t[:, r] = a.T
            if i % 2:
                rr = rows(i // 2)
                new = [cin(h.at[rr], h_hbm.at[rr], 16 + 2 * i), cin(a1.at[rr], a1_hbm.at[rr], 17 + 2 * i)]
                for c in new: c.start()
                cs += new
        c = cin(a1t, a1t_hbm, 3); c.start(); cs.append(c)
        for c in outs() + cs: c.wait()

def fwd(x, dy, wg, wu, wd):
    s = jax.ShapeDtypeStruct((T, D), BF); st = jax.ShapeDtypeStruct((D, T), BF)
    v = pltpu.VMEM((T, D), BF); vt = pltpu.VMEM((D, T), BF)
    return pl.pallas_call(
        fwd_body, grid=(NCH,), name="fwd0",
        out_shape=(s, s, st, s, st, st),
        in_specs=[ANY, ANY, pl.BlockSpec((1, D, C), lambda j: (0, 0, j)), pl.BlockSpec((1, D, C), lambda j: (0, 0, j)), ANY],
        out_specs=[ANY] * 6,
        scratch_shapes=[v, v, v, vt, vt, pltpu.VMEM((T, FF), BF), pltpu.VMEM((FF, D), BF), v, v, vt, pltpu.SemaphoreType.DMA((32,))],
        compiler_params=cparams(dimension_semantics=("arbitrary",)),
    )(x, dy, wg, wu, wd)

U = 2 * NCH
NR2 = 9
STAGE2 = (3, 5, 6, 8, 9, 11, 13, 15, 17)
STAGE3 = (5, 7, 9, 10, 12, 14, 16)
STAGE4 = (7, 9, 12, 14, 16)
MESH = pl.DeviceIdType.MESH

def upto(table, s):
    n = jnp.int32(0)
    for t in table:
        n = n + jnp.where(s >= t, 1, 0)
    return n

def mega_body(a1_hbm, a1t_hbm, dy_hbm, dyt_hbm, h1_hbm, a0_hbm, a0t_hbm, wg_ref, wu_ref, wd_ref, f_hbm,
              a, at, d, dt, acc, hid, dg, du, buf, r0, r1, r2,
              sem, p0s, p0r, s1s, s1r, ms, mr, os_, or_, ps, pr, lf, free):
    s = pl.program_id(0)
    me = lax.axis_index("dp")
    core, z = lax.rem(me, 2), lax.div(me, 2)
    inner = jnp.logical_and(z >= 1, z <= 2)
    outer = jnp.logical_not(inner)
    partner = me + 1 - 2 * core
    up = me + 2 - 4 * lax.div(z, 3)
    mid = me + 6 - 4 * z
    out = me - 6 + 4 * z
    RT = 512

    def local(src, dst, i): return pltpu.make_async_copy(src, dst, sem.at[i])
    def remote(src, dst, ss, rs, dev):
        return pltpu.make_async_remote_copy(src_ref=src, dst_ref=dst, send_sem=ss, recv_sem=rs, device_id={"dp": dev}, device_id_type=MESH)
    def rows(i): return pl.ds(i * RT, RT)

    def cp0(u): return remote(buf.at[lax.rem(u, 2), 1 - core], r0.at[u], p0s.at[u], p0r.at[u], partner)
    def cs1(u): return remote(r0.at[u], r1.at[u], s1s.at[u], s1r.at[u], up)
    def cmid(u): return remote(r0.at[u], r2.at[lax.rem(u, NR2)], ms.at[u], mr.at[u], mid)
    def cout(u): return remote(r1.at[u], f_hbm.at[u, core], os_.at[u], or_.at[u], out)
    def cp4i(u): return remote(r1.at[u], f_hbm.at[u, core], ps.at[u], pr.at[u], partner)
    def cp4o(u): return remote(f_hbm.at[u, core], f_hbm.at[u, core], ps.at[u], pr.at[u], partner)
    def clf(u): return pltpu.make_async_copy(r1.at[u], f_hbm.at[u, core], lf.at[u])

    def plus(dst, x, y):
        def part(k, c):
            r = pl.ds(pl.multiple_of(k * 224, 32), 224)
            dst[r, :] = (x[r, :].astype(F32) + y[r, :].astype(F32)).astype(BF)
            return c
        lax.fori_loop(0, 6, part, 0)

    def stage1(u):
        c = cp0(u)
        c.wait()
        plus(r0.at[u], r0.at[u], buf.at[lax.rem(u, 2), core])
        @pl.when(outer)
        def _(): cs1(u).start()

    def stage2(u, c=0):
        cs1(u).wait_recv()
        plus(r0.at[u], r0.at[u], r1.at[u])
        @pl.when(u >= NR2)
        def _(): pl.semaphore_wait(free, 1)
        cmid(u).start()
        return c

    def stage3(u, c=0):
        cmid(u).wait_recv()
        plus(r1.at[u], r0.at[u], r2.at[lax.rem(u, NR2)])
        @pl.when(u < U - NR2)
        def _(): pl.semaphore_signal(free, inc=1, device_id={"dp": mid}, device_id_type=MESH)
        cout(u).start()
        cp4i(u).start()
        clf(u).start()
        return c

    def stage4(u, c=0):
        cout(u).wait_recv()
        cp4o(u).start()
        return c

    @pl.when(s == 0)
    def _():
        barrier = pltpu.get_barrier_semaphore()
        pl.semaphore_signal(barrier, inc=1, device_id={"dp": partner}, device_id_type=MESH)
        @pl.when(outer)
        def _():
            pl.semaphore_signal(barrier, inc=1, device_id={"dp": up}, device_id_type=MESH)
            pl.semaphore_wait(barrier, 2)
        @pl.when(inner)
        def _():
            pl.semaphore_signal(barrier, inc=1, device_id={"dp": mid}, device_id_type=MESH)
            pl.semaphore_signal(barrier, inc=1, device_id={"dp": out}, device_id_type=MESH)
            pl.semaphore_wait(barrier, 3)
        cs = [local(x, y, i) for i, (x, y) in enumerate(((a1_hbm, a), (dy_hbm, d), (a1t_hbm, at), (dyt_hbm, dt)))]
        for c in cs: c.start()
        acc[...] = jnp.zeros((T, D), F32)
        for c in cs: c.wait()

    @pl.when(s == NCH)
    def _():
        local(h1_hbm, a, 0).start()
        local(a0t_hbm, at, 2).start()
        local(h1_hbm, a, 0).wait()
        def part(i, c):
            r = pl.ds(pl.multiple_of(i * 256, 256), 256)
            g = acc[r, :].astype(BF).astype(F32)
            wide = a[r, :].astype(F32)
            scale = norm_scale(wide)
            n = wide * scale
            v = d[r, :] + (scale * (g - n * jnp.mean(n * g, -1, keepdims=True))).astype(BF)
            d[r, :] = v
            dt[:, r] = v.T
            return c
        lax.fori_loop(0, T // 256, part, 0)
        local(a0_hbm, a, 1).start()
        local(a0t_hbm, at, 2).wait()
        local(a0_hbm, a, 1).wait()

    for i in range(T // RT):
        r = rows(i)
        g = dot(a[r, :], wg_ref[0]); u = dot(a[r, :], wu_ref[0])
        dh = dot(d[r, :], wd_ref[0], NT).astype(BF).astype(F32)
        sg = jax.nn.sigmoid(g)
        sl = g * sg
        hid[r, :] = (sl * u).astype(BF)
        du[r, :] = (dh * sl).astype(BF)
        dg[r, :] = (dh * u * (sg + sl * (1 - sg))).astype(BF)

    @pl.when(s >= 1)
    def _(): stage1(s - 1)
    @pl.when(inner)
    def _():
        lax.fori_loop(upto(STAGE2, s - 1), upto(STAGE2, s), stage2, 0)
        lax.fori_loop(upto(STAGE3, s - 1), upto(STAGE3, s), stage3, 0)
    @pl.when(outer)
    def _():
        lax.fori_loop(upto(STAGE4, s - 1), upto(STAGE4, s), stage4, 0)

    slot = lax.rem(s, 2)
    for tile in range(6):
        lhs, rhs = ((at, dg), (at, du), (dt, hid))[tile // 2]
        half, k = divmod(tile, 3)
        buf[slot, half, pl.ds(k * 448, 448), :] = dot(lhs[pl.ds(tile % 2 * 448, 448), :], rhs[...]).astype(BF)
    cp0(s).start()

    @pl.when(s < NCH)
    def _():
        def part(i, c):
            r = pl.ds(pl.multiple_of(i * RT, RT), RT)
            acc[r, :] += dot(dg[r, :], wg_ref[0], NT) + dot(du[r, :], wu_ref[0], NT)
            return c
        lax.fori_loop(0, T // RT, part, 0)

    @pl.when(s == U - 1)
    def _():
        stage1(s)
        @pl.when(inner)
        def _():
            n2, n3 = len(STAGE2), len(STAGE3)
            def both(u, c):
                stage2(u)
                return stage3(u - (n2 - n3), c)
            lax.fori_loop(n2, U, both, 0)
            lax.fori_loop(U - (n2 - n3), U, stage3, 0)
            def done(u, c):
                cmid(u).wait_send(); cout(u).wait_send(); clf(u).wait()
                cp4i(u).wait_send(); cp4i(u).wait_recv()
                return c
            lax.fori_loop(0, U, done, 0)
        @pl.when(outer)
        def _():
            lax.fori_loop(len(STAGE4), U, stage4, 0)
            def done(u, c):
                cs1(u).wait_send()
                cp4o(u).wait_send(); cp4o(u).wait_recv()
                return c
            lax.fori_loop(0, U, done, 0)

def mega(a1, a1t, dy, dyt, h1, a0, a0t, wg, wu, wd):
    v = pltpu.VMEM((T, D), BF); vt = pltpu.VMEM((D, T), BF); w = pltpu.VMEM((T, C), BF)
    up = pl.BlockSpec((1, D, C), lambda s: (1 - s // NCH, 0, s % NCH)); dn = pl.BlockSpec((1, C, D), lambda s: (1 - s // NCH, s % NCH, 0))
    q = lambda n: pltpu.VMEM((n, HALF, C), BF)
    sems = pltpu.SemaphoreType.DMA((U,))
    return pl.pallas_call(
        mega_body, grid=(U,), name="backward",
        out_shape=jax.ShapeDtypeStruct((U, 2, HALF, C), BF),
        in_specs=[ANY] * 7 + [up, up, dn], out_specs=ANY,
        scratch_shapes=[v, vt, v, vt, pltpu.VMEM((T, D), F32), w, w, w, pltpu.VMEM((2, 2, HALF, C), BF), q(U), q(U), q(NR2),
                        pltpu.SemaphoreType.DMA((4,))] + [sems] * 11 + [pltpu.SemaphoreType.REGULAR],
        compiler_params=pltpu.CompilerParams(vmem_limit_bytes=67043328, dimension_semantics=("arbitrary",), collective_id=0, has_side_effects=True),
    )(a1, a1t, dy, dyt, h1, a0, a0t, wg, wu, wd)

def adamw(w, m, v, g):
    m = 0.9 * m + 0.1 * g
    v = 0.95 * v + 0.05 * g * g
    step = m * lax.rsqrt(v + 1e-8) + 0.1 * w
    return (w - 0.02 * step).astype(BF), m, v

def adam_body(f_ref, *refs):
    ins, outs = refs[:9], refs[9:]
    lo, hi = f_ref[0, 0].astype(F32), f_ref[0, 1].astype(F32)
    gs = (lo[:D], jnp.concatenate([lo[D:], hi[:HALF - D]], 0), hi[HALF - D:].T)
    for k, g in enumerate(gs):
        w, m, v = adamw(ins[k][0].astype(F32), ins[3 + k][0], ins[6 + k][0], g)
        outs[k][0] = w; outs[3 + k][0] = m; outs[6 + k][0] = v

def adam(f, args9):
    up = pl.BlockSpec((1, D, C), lambda s: (1 - s // NCH, 0, s % NCH)); dn = pl.BlockSpec((1, C, D), lambda s: (1 - s // NCH, s % NCH, 0))
    dts = [BF] * 3 + [F32] * 6
    return pl.pallas_call(
        adam_body, grid=(U,), name="adam",
        in_specs=[pl.BlockSpec((1, 2, HALF, C), lambda s: (s, 0, 0, 0))] + [up, up, dn] * 3, out_specs=[up, up, dn] * 3,
        out_shape=[jax.ShapeDtypeStruct((2, FF, D) if k % 3 == 2 else (2, D, FF), dts[k]) for k in range(9)],
        compiler_params=cparams(dimension_semantics=("arbitrary",)),
    )(f, *args9)

from jax.sharding import PartitionSpec as P

def solution(mesh):
    def step(x, dy, *arrays):
        wg, wu, wd = arrays[:3]
        x, dy = x[0], dy[0]
        h1, a1, a1t, a0, a0t, dyt = fwd(x, dy, wg, wu, wd)
        f = mega(a1, a1t, dy, dyt, h1, a0, a0t, wg, wu, wd)
        return tuple(adam(f, arrays))

    return jax.shard_map(
        step,
        mesh=mesh,
        in_specs=(P(("rep", "dp"), None, None),) * 2 + (P(None, None, None),) * 9,
        out_specs=(P("rep", None, None),) * 9,
        check_vma=False,
    )
```

```python
import functools
import jax, jax.numpy as jnp
from jax import lax
from jax.experimental import pallas as pl
from jax.experimental.pallas import tpu as pltpu
BF, F32 = jnp.bfloat16, jnp.float32
T, D, FF = 2048, 896, 2304
C = 256
NCH = FF // C
HALF = 3 * D // 2
VL = 60 * 2**20
NT = (((1,), (1,)), ((), ()))

def dot(a, b, dims=(((1,), (0,)), ((), ()))):
    return lax.dot_general(a, b, dims, preferred_element_type=F32)

def cparams(**kw):
    return pltpu.CompilerParams(vmem_limit_bytes=VL, **kw)

VM = pl.BlockSpec(memory_space=pltpu.VMEM)
ANY = pl.BlockSpec(memory_space=pl.ANY)

def norm_scale(wide):
    return lax.rsqrt(jnp.mean(wide * wide, -1, keepdims=True) + 1e-6)

def fwd_body(x_hbm, dy_hbm, wg_ref, wu_ref, wd_hbm, h_hbm, a1_hbm, a1t_hbm, a0_hbm, a0t_hbm, dyt_hbm,
             x, dy, a0, a0t, dyt, hid, wd, h, a1, a1t, sem):
    j = pl.program_id(0)
    RT = 512
    def cin(src, dst, i): return pltpu.make_async_copy(src, dst, sem.at[i])
    def rows(i): return pl.ds(i * RT, RT)
    outs = lambda: [cin(a0, a0_hbm, 4), cin(a0t, a0t_hbm, 5), cin(dyt, dyt_hbm, 6)]
    @pl.when(j == 0)
    def _():
        for i in range(4):
            cin(x_hbm.at[rows(i)], x.at[rows(i)], 12 + i).start()
        cin(dy_hbm, dy, 1).start()
        cin(wd_hbm.at[0], wd, 2).start()
        for i in range(4):
            cin(x_hbm.at[rows(i)], x.at[rows(i)], 12 + i).wait()
            wide = x[rows(i), :].astype(F32)
            a0[rows(i), :] = (wide * norm_scale(wide)).astype(BF)
        cin(a0, a0_hbm, 4).start()
        cin(dy_hbm, dy, 1).wait()
    cols = pl.ds(pl.multiple_of(j * C, C), C)
    for i in range(4):
        a = a0[rows(i), :]
        g = dot(a, wg_ref[0]); u = dot(a, wu_ref[0])
        hid[rows(i), cols] = (g * jax.nn.sigmoid(g) * u).astype(BF)
    r = pl.ds(pl.multiple_of(jnp.minimum(j, 7) * 256, 256), 256)
    a0t[:, r] = a0[r, :].T
    dyt[:, r] = dy[r, :].T
    @pl.when(j == NCH - 1)
    def _():
        for c in outs()[1:]: c.start()
        cin(wd_hbm.at[0], wd, 2).wait()
        cs = []
        for i in range(8):
            r = pl.ds(i * 256, 256)
            o = dot(hid[r, :], wd[...]).astype(BF)
            y = x[r, :] + o
            h[r, :] = y
            wide = y.astype(F32)
            a = (wide * norm_scale(wide)).astype(BF)
            a1[r, :] = a
            a1t[:, r] = a.T
            if i % 2:
                rr = rows(i // 2)
                new = [cin(h.at[rr], h_hbm.at[rr], 16 + 2 * i), cin(a1.at[rr], a1_hbm.at[rr], 17 + 2 * i)]
                for c in new: c.start()
                cs += new
        c = cin(a1t, a1t_hbm, 3); c.start(); cs.append(c)
        for c in outs() + cs: c.wait()

def fwd(x, dy, wg, wu, wd):
    s = jax.ShapeDtypeStruct((T, D), BF); st = jax.ShapeDtypeStruct((D, T), BF)
    v = pltpu.VMEM((T, D), BF); vt = pltpu.VMEM((D, T), BF)
    return pl.pallas_call(
        fwd_body, grid=(NCH,), name="fwd0",
        out_shape=(s, s, st, s, st, st),
        in_specs=[ANY, ANY, pl.BlockSpec((1, D, C), lambda j: (0, 0, j)), pl.BlockSpec((1, D, C), lambda j: (0, 0, j)), ANY],
        out_specs=[ANY] * 6,
        scratch_shapes=[v, v, v, vt, vt, pltpu.VMEM((T, FF), BF), pltpu.VMEM((FF, D), BF), v, v, vt, pltpu.SemaphoreType.DMA((32,))],
        compiler_params=cparams(dimension_semantics=("arbitrary",)),
    )(x, dy, wg, wu, wd)

U = 2 * NCH
V = 2 * U
SUB = HALF // 2
NR2 = 18
STAGE2 = (2, 3, 3, 4, 5, 5, 6, 7, 7, 8, 9, 9, 9, 10, 11, 12, 13, 14, 14, 15, 16, 17)
STAGE3 = (4, 4, 5, 6, 6, 7, 8, 8, 9, 10, 10, 10, 11, 12, 13, 14, 15, 15, 16, 17)
STAGE4 = (5, 6, 7, 7, 8, 9, 9, 10, 11, 11, 11, 12, 13, 14, 15, 16, 16, 17)
MESH = pl.DeviceIdType.MESH

def upto(table, s):
    n = jnp.int32(0)
    for t in table:
        n = n + jnp.where(s >= t, 1, 0)
    return n

def mega_body(a1_hbm, a1t_hbm, dy_hbm, dyt_hbm, h1_hbm, a0_hbm, a0t_hbm, wg_ref, wu_ref, wd_ref, f_hbm,
              a, at, d, dt, acc, hid, dg, du, buf, r0, r1, r2,
              sem, p0s, p0r, s1s, s1r, ms, mr, os_, or_, ps, pr, lf, free):
    s = pl.program_id(0)
    me = lax.axis_index("dp")
    core, z = lax.rem(me, 2), lax.div(me, 2)
    inner = jnp.logical_and(z >= 1, z <= 2)
    outer = jnp.logical_not(inner)
    partner = me + 1 - 2 * core
    up = me + 2 - 4 * lax.div(z, 3)
    mid = me + 6 - 4 * z
    out = me - 6 + 4 * z
    RT = 512

    def local(src, dst, i): return pltpu.make_async_copy(src, dst, sem.at[i])
    def remote(src, dst, ss, rs, dev):
        return pltpu.make_async_remote_copy(src_ref=src, dst_ref=dst, send_sem=ss, recv_sem=rs, device_id={"dp": dev}, device_id_type=MESH)
    def rows(i): return pl.ds(i * RT, RT)

    def cp0(u): return remote(buf.at[lax.rem(u, 2), 1 - core], r0.at[pl.ds(pl.multiple_of(u * HALF, HALF), HALF)], p0s.at[u], p0r.at[u], partner)
    def at0(p): return r0.at[pl.ds(pl.multiple_of(p * SUB, SUB), SUB)]
    def at1(p): return r1.at[pl.ds(pl.multiple_of(p * SUB, SUB), SUB)]
    def at2(p): return r2.at[pl.ds(pl.multiple_of(lax.rem(p, NR2) * SUB, SUB), SUB)]
    def to(p): return f_hbm.at[lax.div(p, 2), core, pl.ds(pl.multiple_of(lax.rem(p, 2) * SUB, SUB), SUB)]
    def cs1(p): return remote(at0(p), at1(p), s1s.at[p], s1r.at[p], up)
    def cmid(p): return remote(at0(p), at2(p), ms.at[p], mr.at[p], mid)
    def cout(p): return remote(at1(p), to(p), os_.at[p], or_.at[p], out)
    def cp4i(p): return remote(at1(p), to(p), ps.at[p], pr.at[p], partner)
    def cp4o(p): return remote(to(p), to(p), ps.at[p], pr.at[p], partner)
    def clf(p): return pltpu.make_async_copy(at1(p), to(p), lf.at[p])

    def plus(dst, x, y, n):
        def part(k, c):
            r = pl.ds(pl.multiple_of(k * 224, 32), 224)
            dst[r, :] = (x[r, :].astype(F32) + y[r, :].astype(F32)).astype(BF)
            return c
        lax.fori_loop(0, n, part, 0)

    def stage1(u):
        c = cp0(u)
        c.wait()
        whole = r0.at[pl.ds(pl.multiple_of(u * HALF, HALF), HALF)]
        plus(whole, whole, buf.at[lax.rem(u, 2), core], 6)
        @pl.when(outer)
        def _():
            cs1(2 * u).start()
            cs1(2 * u + 1).start()

    def stage2(u, c=0):
        cs1(u).wait_recv()
        plus(at0(u), at0(u), at1(u), 3)
        @pl.when(u >= NR2)
        def _(): pl.semaphore_wait(free, 1)
        cmid(u).start()
        return c

    def stage3(u, c=0):
        cmid(u).wait_recv()
        plus(at1(u), at0(u), at2(u), 3)
        @pl.when(u < V - NR2)
        def _(): pl.semaphore_signal(free, inc=1, device_id={"dp": mid}, device_id_type=MESH)
        cout(u).start()
        cp4i(u).start()
        clf(u).start()
        return c

    def stage4(u, c=0):
        cout(u).wait_recv()
        cp4o(u).start()
        return c

    @pl.when(s == 0)
    def _():
        barrier = pltpu.get_barrier_semaphore()
        pl.semaphore_signal(barrier, inc=1, device_id={"dp": partner}, device_id_type=MESH)
        @pl.when(outer)
        def _():
            pl.semaphore_signal(barrier, inc=1, device_id={"dp": up}, device_id_type=MESH)
            pl.semaphore_wait(barrier, 2)
        @pl.when(inner)
        def _():
            pl.semaphore_signal(barrier, inc=1, device_id={"dp": mid}, device_id_type=MESH)
            pl.semaphore_signal(barrier, inc=1, device_id={"dp": out}, device_id_type=MESH)
            pl.semaphore_wait(barrier, 3)
        cs = [local(x, y, i) for i, (x, y) in enumerate(((a1_hbm, a), (dy_hbm, d), (a1t_hbm, at), (dyt_hbm, dt)))]
        for c in cs: c.start()
        acc[...] = jnp.zeros((T, D), F32)
        for c in cs[:2]: c.wait()

    @pl.when(s == NCH)
    def _():
        local(h1_hbm, a, 0).start()
        local(a0t_hbm, at, 2).start()
        local(h1_hbm, a, 0).wait()
        def part(i, c):
            r = pl.ds(pl.multiple_of(i * 256, 256), 256)
            g = acc[r, :].astype(BF).astype(F32)
            wide = a[r, :].astype(F32)
            scale = norm_scale(wide)
            n = wide * scale
            v = d[r, :] + (scale * (g - n * jnp.mean(n * g, -1, keepdims=True))).astype(BF)
            d[r, :] = v
            dt[:, r] = v.T
            return c
        lax.fori_loop(0, T // 256, part, 0)
        local(a0_hbm, a, 1).start()
        local(a0t_hbm, at, 2).wait()
        local(a0_hbm, a, 1).wait()

    for i in range(T // RT):
        r = rows(i)
        g = dot(a[r, :], wg_ref[0]); u = dot(a[r, :], wu_ref[0])
        dh = dot(d[r, :], wd_ref[0], NT).astype(BF).astype(F32)
        sg = jax.nn.sigmoid(g)
        sl = g * sg
        hid[r, :] = (sl * u).astype(BF)
        du[r, :] = (dh * sl).astype(BF)
        dg[r, :] = (dh * u * (sg + sl * (1 - sg))).astype(BF)

    @pl.when(s == 0)
    def _():
        local(a1t_hbm, at, 2).wait()
        local(dyt_hbm, dt, 3).wait()
    @pl.when(s > NCH)
    def _(): stage1(s - 1)
    @pl.when(inner)
    def _():
        lax.fori_loop(upto(STAGE2, s - 1), upto(STAGE2, s), stage2, 0)
        lax.fori_loop(upto(STAGE3, s - 1), upto(STAGE3, s), stage3, 0)
    @pl.when(outer)
    def _():
        lax.fori_loop(upto(STAGE4, s - 1), upto(STAGE4, s), stage4, 0)

    slot = lax.rem(s, 2)
    for tile in range(6):
        lhs, rhs = ((at, dg), (at, du), (dt, hid))[tile // 2]
        half, k = divmod(tile, 3)
        buf[slot, half, pl.ds(k * 448, 448), :] = dot(lhs[pl.ds(tile % 2 * 448, 448), :], rhs[...]).astype(BF)
    cp0(s).start()

    @pl.when(s < NCH)
    def _():
        def part(i, c):
            r = pl.ds(pl.multiple_of(i * RT, RT), RT)
            acc[r, :] += dot(dg[r, :], wg_ref[0], NT) + dot(du[r, :], wu_ref[0], NT)
            return c
        lax.fori_loop(0, T // RT, part, 0)
        stage1(s)

    @pl.when(s == U - 1)
    def _():
        stage1(s)
        @pl.when(inner)
        def _():
            n2, n3 = len(STAGE2), len(STAGE3)
            lax.fori_loop(n3, n2 - 1, stage3, 0)
            def both(u, c):
                stage2(u)
                return stage3(u - 1, c)
            lax.fori_loop(n2, V, both, 0)
            stage3(V - 1)
            def done(u, c):
                cmid(u).wait_send(); cout(u).wait_send(); clf(u).wait()
                cp4i(u).wait_send(); cp4i(u).wait_recv()
                return c
            lax.fori_loop(0, V, done, 0)
        @pl.when(outer)
        def _():
            lax.fori_loop(len(STAGE4), V, stage4, 0)
            def done(u, c):
                cs1(u).wait_send()
                cp4o(u).wait_send(); cp4o(u).wait_recv()
                return c
            lax.fori_loop(0, V, done, 0)

def mega(a1, a1t, dy, dyt, h1, a0, a0t, wg, wu, wd):
    v = pltpu.VMEM((T, D), BF); vt = pltpu.VMEM((D, T), BF); w = pltpu.VMEM((T, C), BF)
    up = pl.BlockSpec((1, D, C), lambda s: (1 - s // NCH, 0, s % NCH)); dn = pl.BlockSpec((1, C, D), lambda s: (1 - s // NCH, s % NCH, 0))
    q = lambda n: pltpu.VMEM((n * SUB, C), BF)
    sems = pltpu.SemaphoreType.DMA((V,))
    return pl.pallas_call(
        mega_body, grid=(U,), name="backward",
        out_shape=jax.ShapeDtypeStruct((U, 2, HALF, C), BF),
        in_specs=[ANY] * 7 + [up, up, dn], out_specs=ANY,
        scratch_shapes=[v, vt, v, vt, pltpu.VMEM((T, D), F32), w, w, w, pltpu.VMEM((2, 2, HALF, C), BF), q(V), q(V), q(NR2),
                        pltpu.SemaphoreType.DMA((4,))] + [sems] * 11 + [pltpu.SemaphoreType.REGULAR],
        compiler_params=pltpu.CompilerParams(vmem_limit_bytes=67043328, dimension_semantics=("arbitrary",), collective_id=0, has_side_effects=True),
    )(a1, a1t, dy, dyt, h1, a0, a0t, wg, wu, wd)

def adamw(w, m, v, g):
    m = 0.9 * m + 0.1 * g
    v = 0.95 * v + 0.05 * g * g
    step = m * lax.rsqrt(v + 1e-8) + 0.1 * w
    return (w - 0.02 * step).astype(BF), m, v

def adam_body(f_ref, *refs):
    ins, outs = refs[:9], refs[9:]
    lo, hi = f_ref[0, 0].astype(F32), f_ref[0, 1].astype(F32)
    gs = (lo[:D], jnp.concatenate([lo[D:], hi[:HALF - D]], 0), hi[HALF - D:].T)
    for k, g in enumerate(gs):
        w, m, v = adamw(ins[k][0].astype(F32), ins[3 + k][0], ins[6 + k][0], g)
        outs[k][0] = w; outs[3 + k][0] = m; outs[6 + k][0] = v

def adam(f, args9):
    up = pl.BlockSpec((1, D, C), lambda s: (1 - s // NCH, 0, s % NCH)); dn = pl.BlockSpec((1, C, D), lambda s: (1 - s // NCH, s % NCH, 0))
    dts = [BF] * 3 + [F32] * 6
    return pl.pallas_call(
        adam_body, grid=(U,), name="adam",
        in_specs=[pl.BlockSpec((1, 2, HALF, C), lambda s: (s, 0, 0, 0))] + [up, up, dn] * 3, out_specs=[up, up, dn] * 3,
        out_shape=[jax.ShapeDtypeStruct((2, FF, D) if k % 3 == 2 else (2, D, FF), dts[k]) for k in range(9)],
        compiler_params=cparams(dimension_semantics=("arbitrary",)),
    )(f, *args9)

from jax.sharding import PartitionSpec as P

def solution(mesh):
    def step(x, dy, *arrays):
        wg, wu, wd = arrays[:3]
        x, dy = x[0], dy[0]
        h1, a1, a1t, a0, a0t, dyt = fwd(x, dy, wg, wu, wd)
        f = mega(a1, a1t, dy, dyt, h1, a0, a0t, wg, wu, wd)
        return tuple(adam(f, arrays))

    return jax.shard_map(
        step,
        mesh=mesh,
        in_specs=(P(("rep", "dp"), None, None),) * 2 + (P(None, None, None),) * 9,
        out_specs=(P("rep", None, None),) * 9,
        check_vma=False,
    )
```

```python
import functools
import jax, jax.numpy as jnp
from jax import lax
from jax.experimental import pallas as pl
from jax.experimental.pallas import tpu as pltpu
BF, F32 = jnp.bfloat16, jnp.float32
T, D, FF = 2048, 896, 2304
C = 256
NCH = FF // C
CF = 768
NF = FF // CF
HALF = 3 * D // 2
VL = 60 * 2**20
NT = (((1,), (1,)), ((), ()))

def dot(a, b, dims=(((1,), (0,)), ((), ()))):
    return lax.dot_general(a, b, dims, preferred_element_type=F32)

def cparams(**kw):
    return pltpu.CompilerParams(vmem_limit_bytes=VL, **kw)

VM = pl.BlockSpec(memory_space=pltpu.VMEM)
ANY = pl.BlockSpec(memory_space=pl.ANY)

def norm_scale(wide):
    return lax.rsqrt(jnp.mean(wide * wide, -1, keepdims=True) + 1e-6)

def fwd_body(x_hbm, dy_hbm, wg_ref, wu_ref, wd_hbm, h_hbm, a1_hbm, a1t_hbm, a0_hbm, a0t_hbm, dyt_hbm,
             x, dy, a0, a0t, dyt, hid, wd, h, a1, a1t, sem):
    j = pl.program_id(0)
    RT = 512
    def cin(src, dst, i): return pltpu.make_async_copy(src, dst, sem.at[i])
    def rows(i): return pl.ds(i * RT, RT)
    outs = lambda: [cin(a0, a0_hbm, 4), cin(a0t, a0t_hbm, 5), cin(dyt, dyt_hbm, 6)]
    @pl.when(j == 0)
    def _():
        for i in range(4):
            cin(x_hbm.at[rows(i)], x.at[rows(i)], 12 + i).start()
        cin(dy_hbm, dy, 1).start()
        cin(wd_hbm.at[0], wd, 2).start()
        for i in range(4):
            cin(x_hbm.at[rows(i)], x.at[rows(i)], 12 + i).wait()
            wide = x[rows(i), :].astype(F32)
            a0[rows(i), :] = (wide * norm_scale(wide)).astype(BF)
        cin(a0, a0_hbm, 4).start()
        cin(dy_hbm, dy, 1).wait()
    cols = pl.ds(pl.multiple_of(j * CF, CF), CF)
    for i in range(4):
        a = a0[rows(i), :]
        g = dot(a, wg_ref[0]); u = dot(a, wu_ref[0])
        hid[rows(i), cols] = (g * jax.nn.sigmoid(g) * u).astype(BF)
        if i < 3:
            r = pl.ds(pl.multiple_of(jnp.minimum(j * 3 + i, 7) * 256, 256), 256)
            a0t[:, r] = a0[r, :].T
            dyt[:, r] = dy[r, :].T
    @pl.when(j == NF - 1)
    def _():
        for c in outs()[1:]: c.start()
        cin(wd_hbm.at[0], wd, 2).wait()
        cs = []
        for i in range(8):
            r = pl.ds(i * 256, 256)
            o = dot(hid[r, :], wd[...]).astype(BF)
            y = x[r, :] + o
            h[r, :] = y
            wide = y.astype(F32)
            a = (wide * norm_scale(wide)).astype(BF)
            a1[r, :] = a
            a1t[:, r] = a.T
            if i % 2:
                rr = rows(i // 2)
                new = [cin(h.at[rr], h_hbm.at[rr], 16 + 2 * i), cin(a1.at[rr], a1_hbm.at[rr], 17 + 2 * i)]
                for c in new: c.start()
                cs += new
        c = cin(a1t, a1t_hbm, 3); c.start(); cs.append(c)
        for c in outs() + cs: c.wait()

def fwd(x, dy, wg, wu, wd):
    s = jax.ShapeDtypeStruct((T, D), BF); st = jax.ShapeDtypeStruct((D, T), BF)
    v = pltpu.VMEM((T, D), BF); vt = pltpu.VMEM((D, T), BF)
    return pl.pallas_call(
        fwd_body, grid=(NF,), name="fwd0",
        out_shape=(s, s, st, s, st, st),
        in_specs=[ANY, ANY, pl.BlockSpec((1, D, CF), lambda j: (0, 0, j)), pl.BlockSpec((1, D, CF), lambda j: (0, 0, j)), ANY],
        out_specs=[ANY] * 6,
        scratch_shapes=[v, v, v, vt, vt, pltpu.VMEM((T, FF), BF), pltpu.VMEM((FF, D), BF), v, v, vt, pltpu.SemaphoreType.DMA((32,))],
        compiler_params=cparams(dimension_semantics=("arbitrary",)),
    )(x, dy, wg, wu, wd)

U = 2 * NCH
V = 2 * U
SUB = HALF // 2
NR2 = 18
STAGE2 = (1, 2, 2, 3, 4, 4, 5, 5, 6, 6, 7, 8, 8, 9, 9, 9, 10, 11, 12, 12, 13, 14, 15, 15, 16, 17, 17)
STAGE3 = (3, 3, 4, 5, 5, 6, 6, 7, 7, 8, 9, 9, 10, 10, 10, 11, 12, 13, 13, 14, 15, 16, 16, 17)
STAGE4 = (4, 5, 6, 6, 7, 7, 8, 8, 9, 10, 10, 11, 11, 11, 12, 13, 14, 14, 15, 16, 17, 17)
MESH = pl.DeviceIdType.MESH

def upto(table, s):
    n = jnp.int32(0)
    for t in table:
        n = n + jnp.where(s >= t, 1, 0)
    return n

def mega_body(a1_hbm, a1t_hbm, dy_hbm, dyt_hbm, h1_hbm, a0_hbm, a0t_hbm, wg_ref, wu_ref, wd_ref, f_hbm,
              a, at, d, dt, acc, hid, dg, du, buf, r0, r1, r2,
              sem, p0s, p0r, s1s, s1r, ms, mr, os_, or_, ps, pr, lf, free):
    s = pl.program_id(0)
    me = lax.axis_index("dp")
    core, z = lax.rem(me, 2), lax.div(me, 2)
    inner = jnp.logical_and(z >= 1, z <= 2)
    outer = jnp.logical_not(inner)
    partner = me + 1 - 2 * core
    up = me + 2 - 4 * lax.div(z, 3)
    mid = me + 6 - 4 * z
    out = me - 6 + 4 * z
    RT = 512

    def local(src, dst, i): return pltpu.make_async_copy(src, dst, sem.at[i])
    def remote(src, dst, ss, rs, dev):
        return pltpu.make_async_remote_copy(src_ref=src, dst_ref=dst, send_sem=ss, recv_sem=rs, device_id={"dp": dev}, device_id_type=MESH)
    def rows(i): return pl.ds(i * RT, RT)

    def cp0(u): return remote(buf.at[lax.rem(u, 2), 1 - core], r0.at[pl.ds(pl.multiple_of(u * HALF, HALF), HALF)], p0s.at[u], p0r.at[u], partner)
    def at0(p): return r0.at[pl.ds(pl.multiple_of(p * SUB, SUB), SUB)]
    def at1(p): return r1.at[pl.ds(pl.multiple_of(p * SUB, SUB), SUB)]
    def at2(p): return r2.at[pl.ds(pl.multiple_of(lax.rem(p, NR2) * SUB, SUB), SUB)]
    def to(p): return f_hbm.at[lax.div(p, 2), core, pl.ds(pl.multiple_of(lax.rem(p, 2) * SUB, SUB), SUB)]
    def cs1(p): return remote(at0(p), at1(p), s1s.at[p], s1r.at[p], up)
    def cmid(p): return remote(at0(p), at2(p), ms.at[p], mr.at[p], mid)
    def cout(p): return remote(at1(p), to(p), os_.at[p], or_.at[p], out)
    def cp4i(p): return remote(at1(p), to(p), ps.at[p], pr.at[p], partner)
    def cp4o(p): return remote(to(p), to(p), ps.at[p], pr.at[p], partner)
    def clf(p): return pltpu.make_async_copy(at1(p), to(p), lf.at[p])

    def plus(dst, x, y, n):
        def part(k, c):
            r = pl.ds(pl.multiple_of(k * 224, 32), 224)
            dst[r, :] = (x[r, :].astype(F32) + y[r, :].astype(F32)).astype(BF)
            return c
        lax.fori_loop(0, n, part, 0)

    def stage1(u):
        c = cp0(u)
        c.wait()
        whole = r0.at[pl.ds(pl.multiple_of(u * HALF, HALF), HALF)]
        plus(whole, whole, buf.at[lax.rem(u, 2), core], 6)
        @pl.when(outer)
        def _():
            cs1(2 * u).start()
            cs1(2 * u + 1).start()

    def stage2(u, c=0):
        cs1(u).wait_recv()
        plus(at0(u), at0(u), at1(u), 3)
        @pl.when(u >= NR2)
        def _(): pl.semaphore_wait(free, 1)
        cmid(u).start()
        return c

    def stage3(u, c=0):
        cmid(u).wait_recv()
        plus(at1(u), at0(u), at2(u), 3)
        @pl.when(u < V - NR2)
        def _(): pl.semaphore_signal(free, inc=1, device_id={"dp": mid}, device_id_type=MESH)
        cout(u).start()
        cp4i(u).start()
        clf(u).start()
        return c

    def stage4(u, c=0):
        cout(u).wait_recv()
        cp4o(u).start()
        return c

    @pl.when(s == 0)
    def _():
        barrier = pltpu.get_barrier_semaphore()
        pl.semaphore_signal(barrier, inc=1, device_id={"dp": partner}, device_id_type=MESH)
        @pl.when(outer)
        def _():
            pl.semaphore_signal(barrier, inc=1, device_id={"dp": up}, device_id_type=MESH)
            pl.semaphore_wait(barrier, 2)
        @pl.when(inner)
        def _():
            pl.semaphore_signal(barrier, inc=1, device_id={"dp": mid}, device_id_type=MESH)
            pl.semaphore_signal(barrier, inc=1, device_id={"dp": out}, device_id_type=MESH)
            pl.semaphore_wait(barrier, 3)
        cs = [local(x, y, i) for i, (x, y) in enumerate(((a1_hbm, a), (dy_hbm, d), (a1t_hbm, at), (dyt_hbm, dt)))]
        for c in cs: c.start()
        acc[...] = jnp.zeros((T, D), F32)
        for c in cs[:2]: c.wait()

    @pl.when(s == NCH)
    def _():
        local(h1_hbm, a, 0).start()
        local(a0t_hbm, at, 2).start()
        local(h1_hbm, a, 0).wait()
        def part(i, c):
            r = pl.ds(pl.multiple_of(i * 256, 256), 256)
            g = acc[r, :].astype(BF).astype(F32)
            wide = a[r, :].astype(F32)
            scale = norm_scale(wide)
            n = wide * scale
            v = d[r, :] + (scale * (g - n * jnp.mean(n * g, -1, keepdims=True))).astype(BF)
            d[r, :] = v
            dt[:, r] = v.T
            return c
        lax.fori_loop(0, T // 256, part, 0)
        local(a0_hbm, a, 1).start()
        local(a0t_hbm, at, 2).wait()
        local(a0_hbm, a, 1).wait()

    for i in range(T // RT):
        r = rows(i)
        g = dot(a[r, :], wg_ref[0]); u = dot(a[r, :], wu_ref[0])
        dh = dot(d[r, :], wd_ref[0], NT).astype(BF).astype(F32)
        sg = jax.nn.sigmoid(g)
        sl = g * sg
        hid[r, :] = (sl * u).astype(BF)
        du[r, :] = (dh * sl).astype(BF)
        dg[r, :] = (dh * u * (sg + sl * (1 - sg))).astype(BF)

    @pl.when(s == 0)
    def _():
        local(a1t_hbm, at, 2).wait()
        local(dyt_hbm, dt, 3).wait()
    @pl.when(s > NCH)
    def _(): stage1(s - 1)
    @pl.when(inner)
    def _():
        lax.fori_loop(upto(STAGE2, s - 1), upto(STAGE2, s), stage2, 0)
        lax.fori_loop(upto(STAGE3, s - 1), upto(STAGE3, s), stage3, 0)
    @pl.when(outer)
    def _():
        lax.fori_loop(upto(STAGE4, s - 1), upto(STAGE4, s), stage4, 0)

    slot = lax.rem(s, 2)
    for tile in range(6):
        lhs, rhs = ((at, dg), (at, du), (dt, hid))[tile // 2]
        half, k = divmod(tile, 3)
        buf[slot, half, pl.ds(k * 448, 448), :] = dot(lhs[pl.ds(tile % 2 * 448, 448), :], rhs[...]).astype(BF)
    cp0(s).start()

    @pl.when(s < NCH)
    def _():
        def part(i, c):
            r = pl.ds(pl.multiple_of(i * RT, RT), RT)
            acc[r, :] += dot(dg[r, :], wg_ref[0], NT) + dot(du[r, :], wu_ref[0], NT)
            return c
        lax.fori_loop(0, T // RT, part, 0)
        stage1(s)

    @pl.when(s == U - 1)
    def _():
        stage1(s)
        @pl.when(inner)
        def _():
            n2, n3 = len(STAGE2), len(STAGE3)
            lax.fori_loop(n3, n2 - 1, stage3, 0)
            def both(u, c):
                stage2(u)
                return stage3(u - 1, c)
            lax.fori_loop(n2, V, both, 0)
            stage3(V - 1)
            def done(u, c):
                cmid(u).wait_send(); cout(u).wait_send(); clf(u).wait()
                cp4i(u).wait_send(); cp4i(u).wait_recv()
                return c
            lax.fori_loop(0, V, done, 0)
        @pl.when(outer)
        def _():
            lax.fori_loop(len(STAGE4), V, stage4, 0)
            def done(u, c):
                cs1(u).wait_send()
                cp4o(u).wait_send(); cp4o(u).wait_recv()
                return c
            lax.fori_loop(0, V, done, 0)

def mega(a1, a1t, dy, dyt, h1, a0, a0t, wg, wu, wd):
    v = pltpu.VMEM((T, D), BF); vt = pltpu.VMEM((D, T), BF); w = pltpu.VMEM((T, C), BF)
    up = pl.BlockSpec((1, D, C), lambda s: (1 - s // NCH, 0, s % NCH)); dn = pl.BlockSpec((1, C, D), lambda s: (1 - s // NCH, s % NCH, 0))
    q = lambda n: pltpu.VMEM((n * SUB, C), BF)
    sems = pltpu.SemaphoreType.DMA((V,))
    return pl.pallas_call(
        mega_body, grid=(U,), name="backward",
        out_shape=jax.ShapeDtypeStruct((U, 2, HALF, C), BF),
        in_specs=[ANY] * 7 + [up, up, dn], out_specs=ANY,
        scratch_shapes=[v, vt, v, vt, pltpu.VMEM((T, D), F32), w, w, w, pltpu.VMEM((2, 2, HALF, C), BF), q(V), q(V), q(NR2),
                        pltpu.SemaphoreType.DMA((4,))] + [sems] * 11 + [pltpu.SemaphoreType.REGULAR],
        compiler_params=pltpu.CompilerParams(vmem_limit_bytes=67043328, dimension_semantics=("arbitrary",), collective_id=0, has_side_effects=True),
    )(a1, a1t, dy, dyt, h1, a0, a0t, wg, wu, wd)

def adamw(w, m, v, g):
    m = 0.9 * m + 0.1 * g
    v = 0.95 * v + 0.05 * g * g
    step = m * lax.rsqrt(v + 1e-8) + 0.1 * w
    return (w - 0.02 * step).astype(BF), m, v

def adam_body(f_ref, *refs):
    ins, outs = refs[:9], refs[9:]
    lo, hi = f_ref[0, 0].astype(F32), f_ref[0, 1].astype(F32)
    gs = (lo[:D], jnp.concatenate([lo[D:], hi[:HALF - D]], 0), hi[HALF - D:].T)
    for k, g in enumerate(gs):
        w, m, v = adamw(ins[k][0].astype(F32), ins[3 + k][0], ins[6 + k][0], g)
        outs[k][0] = w; outs[3 + k][0] = m; outs[6 + k][0] = v

def adam(f, args9):
    up = pl.BlockSpec((1, D, C), lambda s: (1 - s // NCH, 0, s % NCH)); dn = pl.BlockSpec((1, C, D), lambda s: (1 - s // NCH, s % NCH, 0))
    dts = [BF] * 3 + [F32] * 6
    return pl.pallas_call(
        adam_body, grid=(U,), name="adam",
        in_specs=[pl.BlockSpec((1, 2, HALF, C), lambda s: (s, 0, 0, 0))] + [up, up, dn] * 3, out_specs=[up, up, dn] * 3,
        out_shape=[jax.ShapeDtypeStruct((2, FF, D) if k % 3 == 2 else (2, D, FF), dts[k]) for k in range(9)],
        compiler_params=cparams(dimension_semantics=("arbitrary",)),
    )(f, *args9)

from jax.sharding import PartitionSpec as P

def solution(mesh):
    def step(x, dy, *arrays):
        wg, wu, wd = arrays[:3]
        x, dy = x[0], dy[0]
        h1, a1, a1t, a0, a0t, dyt = fwd(x, dy, wg, wu, wd)
        f = mega(a1, a1t, dy, dyt, h1, a0, a0t, wg, wu, wd)
        return tuple(adam(f, arrays))

    return jax.shard_map(
        step,
        mesh=mesh,
        in_specs=(P(("rep", "dp"), None, None),) * 2 + (P(None, None, None),) * 9,
        out_specs=(P("rep", None, None),) * 9,
        check_vma=False,
    )
```

```python
import functools
import jax, jax.numpy as jnp
from jax import lax
from jax.experimental import pallas as pl
from jax.experimental.pallas import tpu as pltpu
BF, F32 = jnp.bfloat16, jnp.float32
T, D, FF = 2048, 896, 2304
C = 256
NCH = FF // C
CF = 768
NF = FF // CF
HALF = 3 * D // 2
VL = 60 * 2**20
NT = (((1,), (1,)), ((), ()))

def dot(a, b, dims=(((1,), (0,)), ((), ()))):
    return lax.dot_general(a, b, dims, preferred_element_type=F32)

def cparams(**kw):
    return pltpu.CompilerParams(vmem_limit_bytes=VL, **kw)

VM = pl.BlockSpec(memory_space=pltpu.VMEM)
ANY = pl.BlockSpec(memory_space=pl.ANY)

def norm_scale(wide):
    return lax.rsqrt(jnp.mean(wide * wide, -1, keepdims=True) + 1e-6)

def fwd_body(x_hbm, dy_hbm, wg_ref, wu_ref, wd_hbm, h_hbm, a1_hbm, a1t_hbm, a0_hbm, a0t_hbm, dyt_hbm,
             x, dy, a0, a0t, dyt, hid, wd, h, a1, a1t, sem):
    j = pl.program_id(0)
    RT = 512
    def cin(src, dst, i): return pltpu.make_async_copy(src, dst, sem.at[i])
    def rows(i): return pl.ds(i * RT, RT)
    outs = lambda: [cin(a0, a0_hbm, 4), cin(a0t, a0t_hbm, 5), cin(dyt, dyt_hbm, 6)]
    @pl.when(j == 0)
    def _():
        for i in range(4):
            cin(x_hbm.at[rows(i)], x.at[rows(i)], 12 + i).start()
        cin(dy_hbm, dy, 1).start()
        cin(wd_hbm.at[0], wd, 2).start()
        for i in range(4):
            cin(x_hbm.at[rows(i)], x.at[rows(i)], 12 + i).wait()
            wide = x[rows(i), :].astype(F32)
            a0[rows(i), :] = (wide * norm_scale(wide)).astype(BF)
        cin(a0, a0_hbm, 4).start()
        cin(dy_hbm, dy, 1).wait()
    cols = pl.ds(pl.multiple_of(j * CF, CF), CF)
    for i in range(4):
        a = a0[rows(i), :]
        g = dot(a, wg_ref[0]); u = dot(a, wu_ref[0])
        hid[rows(i), cols] = (g * jax.nn.sigmoid(g) * u).astype(BF)
        if i < 3:
            r = pl.ds(pl.multiple_of(jnp.minimum(j * 3 + i, 7) * 256, 256), 256)
            a0t[:, r] = a0[r, :].T
            dyt[:, r] = dy[r, :].T
    @pl.when(j == NF - 1)
    def _():
        for c in outs()[1:]: c.start()
        cin(wd_hbm.at[0], wd, 2).wait()
        cs = []
        for i in range(8):
            r = pl.ds(i * 256, 256)
            o = dot(hid[r, :], wd[...]).astype(BF)
            y = x[r, :] + o
            h[r, :] = y
            wide = y.astype(F32)
            a = (wide * norm_scale(wide)).astype(BF)
            a1[r, :] = a
            a1t[:, r] = a.T
            if i % 2:
                rr = rows(i // 2)
                new = [cin(h.at[rr], h_hbm.at[rr], 16 + 2 * i), cin(a1.at[rr], a1_hbm.at[rr], 17 + 2 * i)]
                for c in new: c.start()
                cs += new
        c = cin(a1t, a1t_hbm, 3); c.start(); cs.append(c)
        for c in outs() + cs: c.wait()

def fwd(x, dy, wg, wu, wd):
    s = jax.ShapeDtypeStruct((T, D), BF); st = jax.ShapeDtypeStruct((D, T), BF)
    v = pltpu.VMEM((T, D), BF); vt = pltpu.VMEM((D, T), BF)
    return pl.pallas_call(
        fwd_body, grid=(NF,), name="fwd0",
        out_shape=(s, s, st, s, st, st),
        in_specs=[ANY, ANY, pl.BlockSpec((1, D, CF), lambda j: (0, 0, j)), pl.BlockSpec((1, D, CF), lambda j: (0, 0, j)), ANY],
        out_specs=[ANY] * 6,
        scratch_shapes=[v, v, v, vt, vt, pltpu.VMEM((T, FF), BF), pltpu.VMEM((FF, D), BF), v, v, vt, pltpu.SemaphoreType.DMA((32,))],
        compiler_params=cparams(dimension_semantics=("arbitrary",)),
    )(x, dy, wg, wu, wd)

U = 2 * NCH
V = 2 * U
SUB = HALF // 2
NR2 = 18
STAGE2 = (4, 5, 6, 8, 9, 10, 12, 13, 14, 16, 17, 18, 18, 20, 22, 24, 26, 27, 28, 30, 32, 34)
STAGE3 = (6, 7, 9, 10, 11, 13, 14, 15, 17, 18, 19, 19, 21, 23, 25, 27, 28, 29, 31, 33, 35)
MESH = pl.DeviceIdType.MESH

def upto(table, s):
    n = jnp.int32(0)
    for t in table:
        n = n + jnp.where(s >= t, 1, 0)
    return n

def mega_body(a1_hbm, a1t_hbm, dy_hbm, dyt_hbm, h1_hbm, a0_hbm, a0t_hbm, wg_ref, wu_ref, wd_ref, f_hbm,
              a, at, d, dt, acc, hid, dg, du, buf, r0, r1, r2,
              sem, p0s, p0r, s1s, s1r, ms, mr, os_, or_, ps, pr, lf, free):
    s = pl.program_id(0)
    me = lax.axis_index("dp")
    core, z = lax.rem(me, 2), lax.div(me, 2)
    inner = jnp.logical_and(z >= 1, z <= 2)
    outer = jnp.logical_not(inner)
    partner = me + 1 - 2 * core
    up = me + 2 - 4 * lax.div(z, 3)
    mid = me + 6 - 4 * z
    out = me - 6 + 4 * z
    RT = 512

    def local(src, dst, i): return pltpu.make_async_copy(src, dst, sem.at[i])
    def remote(src, dst, ss, rs, dev):
        return pltpu.make_async_remote_copy(src_ref=src, dst_ref=dst, send_sem=ss, recv_sem=rs, device_id={"dp": dev}, device_id_type=MESH)
    def rows(i): return pl.ds(i * RT, RT)

    def cp0(u): return remote(buf.at[lax.rem(u, 2), 1 - core], r0.at[pl.ds(pl.multiple_of(u * HALF, HALF), HALF)], p0s.at[u], p0r.at[u], partner)
    def at0(p): return r0.at[pl.ds(pl.multiple_of(p * SUB, SUB), SUB)]
    def at1(p): return r1.at[pl.ds(pl.multiple_of(p * SUB, SUB), SUB)]
    def at2(p): return r2.at[pl.ds(pl.multiple_of(lax.rem(p, NR2) * SUB, SUB), SUB)]
    def to(p): return f_hbm.at[lax.div(p, 2), core, pl.ds(pl.multiple_of(lax.rem(p, 2) * SUB, SUB), SUB)]
    def cs1(p): return remote(at0(p), at1(p), s1s.at[p], s1r.at[p], up)
    def cmid(p): return remote(at0(p), at2(p), ms.at[p], mr.at[p], mid)
    def cout(p): return remote(at1(p), to(p), os_.at[p], or_.at[p], out)
    def cp4i(p): return remote(at1(p), to(p), ps.at[p], pr.at[p], partner)
    def cp4o(p): return remote(to(p), to(p), ps.at[p], pr.at[p], partner)
    def clf(p): return pltpu.make_async_copy(at1(p), to(p), lf.at[p])

    def plus(dst, x, y, n):
        def part(k, c):
            r = pl.ds(pl.multiple_of(k * 224, 32), 224)
            dst[r, :] = (x[r, :].astype(F32) + y[r, :].astype(F32)).astype(BF)
            return c
        lax.fori_loop(0, n, part, 0)

    def stage1(u):
        c = cp0(u)
        c.wait()
        whole = r0.at[pl.ds(pl.multiple_of(u * HALF, HALF), HALF)]
        plus(whole, whole, buf.at[lax.rem(u, 2), core], 6)
        @pl.when(outer)
        def _():
            cs1(2 * u).start()
            cs1(2 * u + 1).start()

    def stage2(u, c=0):
        cs1(u).wait_recv()
        plus(at0(u), at0(u), at1(u), 3)
        @pl.when(u >= NR2)
        def _(): pl.semaphore_wait(free, 1)
        cmid(u).start()
        return c

    def stage3(u, c=0):
        cmid(u).wait_recv()
        plus(at1(u), at0(u), at2(u), 3)
        @pl.when(u < V - NR2)
        def _(): pl.semaphore_signal(free, inc=1, device_id={"dp": mid}, device_id_type=MESH)
        cout(u).start()
        cp4i(u).start()
        clf(u).start()
        return c

    def stage4(u, c=0):
        cout(u).wait_recv()
        cp4o(u).start()
        return c

    @pl.when(s == 0)
    def _():
        barrier = pltpu.get_barrier_semaphore()
        pl.semaphore_signal(barrier, inc=1, device_id={"dp": partner}, device_id_type=MESH)
        @pl.when(outer)
        def _():
            pl.semaphore_signal(barrier, inc=1, device_id={"dp": up}, device_id_type=MESH)
            pl.semaphore_wait(barrier, 2)
        @pl.when(inner)
        def _():
            pl.semaphore_signal(barrier, inc=1, device_id={"dp": mid}, device_id_type=MESH)
            pl.semaphore_signal(barrier, inc=1, device_id={"dp": out}, device_id_type=MESH)
            pl.semaphore_wait(barrier, 3)
        cs = [local(x, y, i) for i, (x, y) in enumerate(((a1_hbm, a), (dy_hbm, d), (a1t_hbm, at), (dyt_hbm, dt)))]
        for c in cs: c.start()
        acc[...] = jnp.zeros((T, D), F32)
        for c in cs[:2]: c.wait()

    @pl.when(s == NCH)
    def _():
        local(h1_hbm, a, 0).start()
        local(a0t_hbm, at, 2).start()
        local(h1_hbm, a, 0).wait()
        def part(i, c):
            r = pl.ds(pl.multiple_of(i * 256, 256), 256)
            g = acc[r, :].astype(BF).astype(F32)
            wide = a[r, :].astype(F32)
            scale = norm_scale(wide)
            n = wide * scale
            v = d[r, :] + (scale * (g - n * jnp.mean(n * g, -1, keepdims=True))).astype(BF)
            d[r, :] = v
            dt[:, r] = v.T
            return c
        lax.fori_loop(0, T // 256, part, 0)
        local(a0_hbm, a, 1).start()
        local(a0t_hbm, at, 2).wait()
        local(a0_hbm, a, 1).wait()

    for i in range(T // RT):
        r = rows(i)
        g = dot(a[r, :], wg_ref[0]); u = dot(a[r, :], wu_ref[0])
        dh = dot(d[r, :], wd_ref[0], NT).astype(BF).astype(F32)
        sg = jax.nn.sigmoid(g)
        sl = g * sg
        hid[r, :] = (sl * u).astype(BF)
        du[r, :] = (dh * sl).astype(BF)
        dg[r, :] = (dh * u * (sg + sl * (1 - sg))).astype(BF)

    @pl.when(s == 0)
    def _():
        local(a1t_hbm, at, 2).wait()
        local(dyt_hbm, dt, 3).wait()
    @pl.when(s > NCH)
    def _(): stage1(s - 1)
    @pl.when(inner)
    def _():
        lax.fori_loop(upto(STAGE2, 2 * s - 1), upto(STAGE2, 2 * s), stage2, 0)
        lax.fori_loop(upto(STAGE3, 2 * s - 1), upto(STAGE3, 2 * s), stage3, 0)

    slot = lax.rem(s, 2)
    for tile in range(6):
        lhs, rhs = ((at, dg), (at, du), (dt, hid))[tile // 2]
        half, k = divmod(tile, 3)
        buf[slot, half, pl.ds(k * 448, 448), :] = dot(lhs[pl.ds(tile % 2 * 448, 448), :], rhs[...]).astype(BF)
    cp0(s).start()

    @pl.when(s < NCH)
    def _():
        def part(i, c):
            r = pl.ds(pl.multiple_of(i * RT, RT), RT)
            acc[r, :] += dot(dg[r, :], wg_ref[0], NT) + dot(du[r, :], wu_ref[0], NT)
            return c
        lax.fori_loop(0, T // RT, part, 0)
        stage1(s)

    @pl.when(inner)
    def _():
        lax.fori_loop(upto(STAGE2, 2 * s), upto(STAGE2, 2 * s + 1), stage2, 0)
        lax.fori_loop(upto(STAGE3, 2 * s), upto(STAGE3, 2 * s + 1), stage3, 0)

    @pl.when(s == U - 1)
    def _():
        stage1(s)
        @pl.when(inner)
        def _():
            n2, n3 = len(STAGE2), len(STAGE3)
            lax.fori_loop(n3, n2 - 1, stage3, 0)
            def both(u, c):
                stage2(u)
                return stage3(u - 1, c)
            lax.fori_loop(n2, V, both, 0)
            stage3(V - 1)
            def done(u, c):
                cmid(u).wait_send(); cout(u).wait_send(); clf(u).wait()
                cp4i(u).wait_send(); cp4i(u).wait_recv()
                return c
            lax.fori_loop(0, V, done, 0)
        @pl.when(outer)
        def _():
            lax.fori_loop(0, V, stage4, 0)
            def done(u, c):
                cs1(u).wait_send()
                cp4o(u).wait_send(); cp4o(u).wait_recv()
                return c
            lax.fori_loop(0, V, done, 0)

def mega(a1, a1t, dy, dyt, h1, a0, a0t, wg, wu, wd):
    v = pltpu.VMEM((T, D), BF); vt = pltpu.VMEM((D, T), BF); w = pltpu.VMEM((T, C), BF)
    up = pl.BlockSpec((1, D, C), lambda s: (1 - s // NCH, 0, s % NCH)); dn = pl.BlockSpec((1, C, D), lambda s: (1 - s // NCH, s % NCH, 0))
    q = lambda n: pltpu.VMEM((n * SUB, C), BF)
    sems = pltpu.SemaphoreType.DMA((V,))
    return pl.pallas_call(
        mega_body, grid=(U,), name="backward",
        out_shape=jax.ShapeDtypeStruct((U, 2, HALF, C), BF),
        in_specs=[ANY] * 7 + [up, up, dn], out_specs=ANY,
        scratch_shapes=[v, vt, v, vt, pltpu.VMEM((T, D), F32), w, w, w, pltpu.VMEM((2, 2, HALF, C), BF), q(V), q(V), q(NR2),
                        pltpu.SemaphoreType.DMA((4,))] + [sems] * 11 + [pltpu.SemaphoreType.REGULAR],
        compiler_params=pltpu.CompilerParams(vmem_limit_bytes=67043328, dimension_semantics=("arbitrary",), collective_id=0, has_side_effects=True),
    )(a1, a1t, dy, dyt, h1, a0, a0t, wg, wu, wd)

def adamw(w, m, v, g):
    m = 0.9 * m + 0.1 * g
    v = 0.95 * v + 0.05 * g * g
    step = m * lax.rsqrt(v + 1e-8) + 0.1 * w
    return (w - 0.02 * step).astype(BF), m, v

def adam_body(f_ref, *refs):
    ins, outs = refs[:9], refs[9:]
    lo, hi = f_ref[0, 0].astype(F32), f_ref[0, 1].astype(F32)
    gs = (lo[:D], jnp.concatenate([lo[D:], hi[:HALF - D]], 0), hi[HALF - D:].T)
    for k, g in enumerate(gs):
        w, m, v = adamw(ins[k][0].astype(F32), ins[3 + k][0], ins[6 + k][0], g)
        outs[k][0] = w; outs[3 + k][0] = m; outs[6 + k][0] = v

def adam(f, args9):
    up = pl.BlockSpec((1, D, C), lambda s: (1 - s // NCH, 0, s % NCH)); dn = pl.BlockSpec((1, C, D), lambda s: (1 - s // NCH, s % NCH, 0))
    dts = [BF] * 3 + [F32] * 6
    return pl.pallas_call(
        adam_body, grid=(U,), name="adam",
        in_specs=[pl.BlockSpec((1, 2, HALF, C), lambda s: (s, 0, 0, 0))] + [up, up, dn] * 3, out_specs=[up, up, dn] * 3,
        out_shape=[jax.ShapeDtypeStruct((2, FF, D) if k % 3 == 2 else (2, D, FF), dts[k]) for k in range(9)],
        compiler_params=cparams(dimension_semantics=("arbitrary",)),
    )(f, *args9)

from jax.sharding import PartitionSpec as P

def solution(mesh):
    def step(x, dy, *arrays):
        wg, wu, wd = arrays[:3]
        x, dy = x[0], dy[0]
        h1, a1, a1t, a0, a0t, dyt = fwd(x, dy, wg, wu, wd)
        f = mega(a1, a1t, dy, dyt, h1, a0, a0t, wg, wu, wd)
        return tuple(adam(f, arrays))

    return jax.shard_map(
        step,
        mesh=mesh,
        in_specs=(P(("rep", "dp"), None, None),) * 2 + (P(None, None, None),) * 9,
        out_specs=(P("rep", None, None),) * 9,
        check_vma=False,
    )
```
